32 devices in a mesh: dp: 2 (over y), expert: 16 (over z, x, core).
Axes of the slice: x: 2, y: 2, z: 4, core: 2. Of those that a mesh axis runs over, the one named last changes fastest.
Arguments:
- tokens: bfloat16 [512, 4096], P(('dp', 'expert')), may hold values from -6 to 6
- routing: int32 [512, 2], P(('dp', 'expert')), may hold values from 0 to 7, as said below
- hidden_grad: bfloat16 [2048, 4096], P(('dp', 'expert')), may hold values from -3 to 3
- gate_weight: bfloat16 [4096, 65536], P(None, 'expert'), may hold values from -0.09375 to 0.09375
- up_weight: bfloat16 [4096, 65536], P(None, 'expert'), may hold values from -0.09375 to 0.09375
Outputs:
- token_grad: bfloat16 [512, 4096], P(('dp', 'expert'))
- gate_weight_grad: bfloat16 [4096, 65536], P('dp', 'expert')
- up_weight_grad: bfloat16 [4096, 65536], P('dp', 'expert')
The draws below stay inside these ranges and needn't reach their ends.
Inputs may be any that keep to these rules, and one draw needn't show every extreme that they name: `routing`: the 2 entries of a token differ, and no device names one expert in more than 4 of its tokens.
All inputs are finite; a program needn't handle non-finite values.
Results may differ from the reference program's by a relative error of at most 0.0085.
Values may be sent and summed in bfloat16 or wider, within the bound.
A program may use at most 256 MiB of HBM per device.

```python
import jax
import jax.numpy as jnp
from jax import lax

D = 4096
EXPERTS = 8
TOP = 2
FF = 8192
CAP = 4
TOK = 16
FFD = 4096
ROWS = 64
TOKENS = 512
N_DP = 2
N_EXPERT = 16
DEVICES = 32


def draw_routing(key, part):
    hot_expert = jax.random.randint(jax.random.fold_in(key, 11), (), 0, EXPERTS)
    block_keys = jax.random.split(jax.random.fold_in(key, 12), TOKENS // TOK)

    def one_block(block_key):
        key_order, key_cycle, key_offset, key_flip = jax.random.split(block_key, 4)
        order = jax.random.permutation(key_order, TOK)
        token_rank = jnp.argsort(order, stable=True).astype(jnp.int32)
        cycle = jax.random.permutation(key_cycle, EXPERTS - 1).astype(jnp.int32)
        offset = jax.random.randint(key_offset, (), 0, EXPERTS - 1)
        flipped = jax.random.randint(key_flip, (TOK,), 0, 2)
        first_index = token_rank + jnp.maximum(token_rank - CAP, 0)

        def other_expert(index):
            return (hot_expert + 1 + cycle[(index + offset) % (EXPERTS - 1)]) % EXPERTS
        first_other = other_expert(first_index)
        second_other = other_expert(first_index + 1)
        is_hot = token_rank < CAP
        column_a = jnp.where(is_hot, jnp.where(flipped == 1, hot_expert, first_other), first_other)
        column_b = jnp.where(is_hot, jnp.where(flipped == 1, first_other, hot_expert), second_other)
        return jnp.stack([column_a, column_b], axis=1)
    return jax.vmap(one_block)(block_keys).reshape(TOKENS, TOP).astype(jnp.int32)


def level_of(own_key, extent, cuts, least, top_value):
    gain = 1.0
    for axis_at, shards_of in cuts:
        steps = jax.random.uniform(jax.random.fold_in(jax.random.fold_in(own_key, 6), axis_at), (shards_of,), jnp.float32, least / len(cuts), top_value / len(cuts))
        gain = gain * jnp.repeat(jnp.exp(steps), extent[axis_at] // shards_of).reshape((-1,) + (1,) * (len(extent) - 1 - axis_at))
    return gain


def normal_values(rng, dims, deviation, limit, pieces=(), held_as=jnp.bfloat16):
    values = jax.random.normal(rng, dims, jnp.float32) * deviation
    if len(pieces) > 0:
        values = level_of(rng, dims, pieces, -0.22, 0.18) * values
    return jnp.clip(values, min=-limit, max=limit).astype(held_as)


def setup_inputs(seed: int = 0) -> dict:
    arg_keys = jax.random.split(jax.random.key(seed), 6)
    tokens = normal_values(arg_keys[0], (TOKENS, D), 1.0, 6.0, ((0, 32),))
    routing = draw_routing(jax.random.fold_in(arg_keys[5], 71), 0)
    hidden_grad = normal_values(arg_keys[2], (DEVICES * ROWS, FFD), 0.5, 3.0, ((0, 32),))
    gate_weight = normal_values(arg_keys[3], (D, EXPERTS * FF), D ** -0.5, 0.09375, ((1, 16),))
    up_weight = normal_values(arg_keys[4], (D, EXPERTS * FF), D ** -0.5, 0.09375, ((1, 16),))
    return dict(tokens=tokens, routing=routing, hidden_grad=hidden_grad, gate_weight=gate_weight, up_weight=up_weight)


def slot_tables(routing_dev):
    flat_experts = routing_dev.reshape(-1)
    onehot = (flat_experts[:, None] == jnp.arange(EXPERTS, dtype=jnp.int32)[None, :]).astype(jnp.int32)
    before = jnp.cumsum(onehot, axis=0) - onehot
    slot_index = jnp.sum(before * onehot, axis=1)
    target = flat_experts * CAP + slot_index
    placed = target[:, None] == jnp.arange(EXPERTS * CAP, dtype=jnp.int32)[None, :]
    return placed.astype(jnp.float32)


def reference(tokens, routing, hidden_grad, gate_weight, up_weight):
    shards = N_EXPERT // EXPERTS
    ffd_cols = FF // shards
    row_count = N_EXPERT * CAP
    token_blocks = tokens.reshape(N_DP, N_EXPERT, TOK, D)
    route_blocks = routing.reshape(N_DP, N_EXPERT, TOK, TOP)
    placed = jax.vmap(jax.vmap(slot_tables))(route_blocks)
    doubled = jnp.repeat(token_blocks, TOP, axis=2).astype(jnp.float32)
    outgoing = jnp.einsum('rsae,rsad->rsed', placed, doubled, precision=lax.Precision.HIGHEST)
    outgoing = outgoing.astype(jnp.bfloat16).reshape(N_DP, N_EXPERT, EXPERTS, CAP, D)
    expert_inputs = outgoing.transpose(2, 0, 1, 3, 4).reshape(EXPERTS, N_DP, row_count, D)
    grad_blocks = hidden_grad.reshape(N_DP, EXPERTS, shards, row_count, ffd_cols).transpose(1, 0, 2, 3, 4)
    gate_blocks = gate_weight.reshape(D, EXPERTS, FF).transpose(1, 0, 2)
    up_blocks = up_weight.reshape(D, EXPERTS, FF).transpose(1, 0, 2)

    def one_expert(inputs):
        expert_x, expert_h, w_gate, w_up = inputs
        gate_total = jnp.zeros((D, FF), jnp.float32)
        up_total = jnp.zeros((D, FF), jnp.float32)
        sums = []
        for replica in range(N_DP):
            expert_rows = expert_x[replica]
            gate_pre = jnp.dot(expert_rows, w_gate, preferred_element_type=jnp.float32)
            up_pre = jnp.dot(expert_rows, w_up, preferred_element_type=jnp.float32)
            grad_h = expert_h[replica].transpose(1, 0, 2).reshape(row_count, FF).astype(jnp.float32)
            sigmoid_gate = jax.nn.sigmoid(gate_pre)
            gate_grad = (grad_h * up_pre * sigmoid_gate * (1.0 + gate_pre * (1.0 - sigmoid_gate))).astype(jnp.bfloat16)
            up_grad = (grad_h * gate_pre * sigmoid_gate).astype(jnp.bfloat16)
            first_part = jnp.einsum('rsf,dsf->srd', gate_grad.reshape(row_count, shards, ffd_cols).astype(jnp.float32),
                                    w_gate.reshape(D, shards, ffd_cols).astype(jnp.float32))
            second_part = jnp.einsum('rsf,dsf->srd', up_grad.reshape(row_count, shards, ffd_cols).astype(jnp.float32),
                                     w_up.reshape(D, shards, ffd_cols).astype(jnp.float32))
            partial_value = (first_part + second_part).astype(jnp.bfloat16).astype(jnp.float32)
            sums.append(jnp.sum(partial_value, axis=0))
            gate_term = jnp.dot(expert_rows.T, gate_grad, preferred_element_type=jnp.float32)
            up_term = jnp.dot(expert_rows.T, up_grad, preferred_element_type=jnp.float32)
            gate_total = gate_total + gate_term.astype(jnp.bfloat16).astype(jnp.float32)
            up_total = up_total + up_term.astype(jnp.bfloat16).astype(jnp.float32)
        return jnp.stack(sums), gate_total.astype(jnp.bfloat16), up_total.astype(jnp.bfloat16)

    partial_sums, gate_grads, up_grads = lax.map(one_expert, (expert_inputs, grad_blocks, gate_blocks, up_blocks))
    back = partial_sums.reshape(EXPERTS, N_DP, N_EXPERT, CAP, D).transpose(1, 2, 0, 3, 4)
    back = back.reshape(N_DP, N_EXPERT, EXPERTS * CAP, D)
    gathered = jnp.einsum('rsae,rsed->rsad', placed, back, precision=lax.Precision.HIGHEST)
    token_grad = jnp.sum(gathered.reshape(N_DP, N_EXPERT, TOK, TOP, D), axis=3).astype(jnp.bfloat16)
    token_grad = token_grad.reshape(TOKENS, D)
    gate_weight_grad = gate_grads.transpose(1, 0, 2).reshape(D, EXPERTS * FF)
    up_weight_grad = up_grads.transpose(1, 0, 2).reshape(D, EXPERTS * FF)
    return token_grad, gate_weight_grad, up_weight_grad
```

```python
import functools

import jax
import jax.numpy as jnp
from jax import lax
from jax.experimental import pallas as pl
from jax.experimental.pallas import tpu as pltpu
from jax.sharding import PartitionSpec as P


EXPERTS = 8
TOP = 2
CAP = 4


def from_partner(block, axis, apart):
    count = lax.axis_size(axis)
    route = []
    for low in range(count):
        high = low | 1 << apart
        if high != low and high < count:
            route += [(low, high), (high, low)]
    return lax.ppermute(block, axis, route)


def slot_tables(routing_dev):
    flat_experts = routing_dev.reshape(-1)
    onehot = (flat_experts[:, None] == jnp.arange(EXPERTS, dtype=jnp.int32)[None, :]).astype(
        jnp.int32
    )
    before = jnp.cumsum(onehot, axis=0) - onehot
    slot_index = jnp.sum(before * onehot, axis=1)
    target = flat_experts * CAP + slot_index
    placed = target[:, None] == jnp.arange(EXPERTS * CAP, dtype=jnp.int32)[None, :]
    return placed.astype(jnp.float32)


PIECES = 2
BLOCK = 512
WEIGHT_BLOCK = 256
TRANSPOSED = (((1,), (1,)), ((), ()))


def hidden_kernel(steps, first, *refs):
    if first:
        rows_ref, h_ref, gate_ref, up_ref, grads_ref, out_ref, total_ref = refs
    else:
        rows_ref, h_ref, gate_ref, up_ref, before_ref, grads_ref, out_ref, total_ref = refs
    step = pl.program_id(0)

    @pl.when(step == 0)
    def _():
        total_ref[...] = jnp.zeros_like(total_ref) if first else before_ref[...]

    rows = rows_ref[...]
    gate_pre = jnp.dot(rows, gate_ref[...], preferred_element_type=jnp.float32)
    up_pre = jnp.dot(rows, up_ref[...], preferred_element_type=jnp.float32)
    grad_h = h_ref[...].astype(jnp.float32)
    sig = jax.nn.sigmoid(gate_pre)
    gate_grad = (grad_h * up_pre * sig * (1.0 + gate_pre * (1.0 - sig))).astype(jnp.bfloat16)
    up_grad = (grad_h * gate_pre * sig).astype(jnp.bfloat16)
    grads_ref[0] = gate_grad
    grads_ref[1] = up_grad
    back = lax.dot_general(
        gate_grad, gate_ref[...], TRANSPOSED, preferred_element_type=jnp.float32
    ) + lax.dot_general(up_grad, up_ref[...], TRANSPOSED, preferred_element_type=jnp.float32)
    total_ref[...] += back

    @pl.when(step == steps - 1)
    def _():
        out_ref[...] = total_ref[...].astype(out_ref.dtype)


def hidden_pass(piece, pieces, block, rows, hidden, gate_weight, up_weight, before):
    count, width = rows.shape
    span = gate_weight.shape[1] // pieces
    steps = span // block
    first, last = piece == 0, piece == pieces - 1
    offset = piece * steps
    whole = pl.BlockSpec((count, width), lambda j: (0, 0))
    in_specs = [
        whole,
        pl.BlockSpec((count, block), lambda j: (0, offset + j)),
        pl.BlockSpec((width, block), lambda j: (0, offset + j)),
        pl.BlockSpec((width, block), lambda j: (0, offset + j)),
    ]
    args = [rows, hidden, gate_weight, up_weight]
    if not first:
        in_specs.append(whole)
        args.append(before)
    return pl.pallas_call(
        functools.partial(hidden_kernel, steps, first),
        grid=(steps,),
        in_specs=in_specs,
        out_specs=[pl.BlockSpec((2, count, block), lambda j: (0, 0, j)), whole],
        out_shape=[
            jax.ShapeDtypeStruct((2, count, span), jnp.bfloat16),
            jax.ShapeDtypeStruct((count, width), jnp.bfloat16 if last else jnp.float32),
        ],
        scratch_shapes=[pltpu.VMEM((count, width), jnp.float32)],
        cost_estimate=pl.CostEstimate(
            flops=8 * count * width * span,
            bytes_accessed=4 * width * span,
            transcendentals=count * span,
        ),
        compiler_params=pltpu.CompilerParams(
            dimension_semantics=("arbitrary",), vmem_limit_bytes=40 * 1024 * 1024
        ),
    )(*args)


def weight_kernel(*refs):
    own_ref, their_ref, own_grads, their_grads = refs[:4]
    gate_ref, up_ref, turned_ref = refs[-3:]

    @pl.when(pl.program_id(0) == 0)
    def _():
        both = jnp.concatenate([own_ref[...], their_ref[...]], axis=0)
        turned_ref[...] = both.T

    for at, out_ref in ((0, gate_ref), (1, up_ref)):
        grads = jnp.concatenate([own_grads[at], their_grads[at]], axis=0)
        out_ref[...] = jnp.dot(
            turned_ref[...], grads, preferred_element_type=jnp.float32
        ).astype(out_ref.dtype)


def weight_pass(piece, pieces, block, own, their, own_grads, their_grads, before):
    count, half = own.shape
    span = own_grads.shape[2]
    steps = span // block
    offset = piece * steps
    columns = pl.BlockSpec((count, half), lambda j: (0, 0))
    grads = pl.BlockSpec((2, count, block), lambda j: (0, 0, j))
    in_specs = [columns, columns, grads, grads]
    args = [own, their, own_grads, their_grads]
    aliases = {}
    if before is not None:
        in_specs += [pl.BlockSpec(memory_space=pl.ANY)] * 2
        args += list(before)
        aliases = {4: 0, 5: 1}
    result = jax.ShapeDtypeStruct((half, span * pieces), jnp.bfloat16)
    out = pl.BlockSpec((half, block), lambda j: (0, offset + j))
    return pl.pallas_call(
        weight_kernel,
        grid=(steps,),
        in_specs=in_specs,
        out_specs=[out, out],
        out_shape=[result, result],
        scratch_shapes=[pltpu.VMEM((half, 2 * count), jnp.bfloat16)],
        input_output_aliases=aliases,
        cost_estimate=pl.CostEstimate(
            flops=8 * count * half * span,
            bytes_accessed=4 * half * span,
            transcendentals=0,
        ),
        compiler_params=pltpu.CompilerParams(
            dimension_semantics=("arbitrary",), vmem_limit_bytes=40 * 1024 * 1024
        ),
    )(*args)


def layer(tokens, routing, hidden_grad, gate_weight, up_weight):
    token_count = tokens.shape[0]
    model_width = tokens.shape[1]
    ffd_cols = gate_weight.shape[1]
    shards = lax.axis_size("expert") // EXPERTS
    placed = slot_tables(routing)
    doubled = jnp.repeat(tokens, TOP, axis=0)
    outgoing = jnp.dot(
        placed.T.astype(jnp.bfloat16), doubled, preferred_element_type=jnp.float32
    ).astype(jnp.bfloat16)
    copies = jnp.broadcast_to(
        outgoing.reshape(EXPERTS, 1, CAP, model_width), (EXPERTS, shards, CAP, model_width)
    )
    copies = copies.reshape(EXPERTS * shards, CAP, model_width)
    arrived = lax.all_to_all(copies, "expert", split_axis=0, concat_axis=0, tiled=True)
    expert_rows = arrived.reshape(-1, model_width)
    half_width = model_width // lax.axis_size("dp")
    replica_index = lax.axis_index("dp")
    own_columns = lax.dynamic_slice_in_dim(expert_rows, replica_index * half_width, half_width, 1)
    far_columns = lax.dynamic_slice_in_dim(
        expert_rows, (1 - replica_index) * half_width, half_width, 1
    )
    their_columns = from_partner(far_columns, "dp", 0)
    pieces = PIECES
    block = min(BLOCK, ffd_cols // pieces)
    weight_block = min(WEIGHT_BLOCK, ffd_cols // pieces)
    partial_value = None
    pairs = []
    for piece in range(pieces):
        grads, partial_value = hidden_pass(
            piece, pieces, block, expert_rows, hidden_grad, gate_weight, up_weight, partial_value
        )
        pairs.append((grads, from_partner(grads, "dp", 0)))
    returned = lax.all_to_all(
        partial_value.reshape(-1, CAP, model_width),
        "expert",
        split_axis=0,
        concat_axis=0,
        tiled=True,
    )
    summed = jnp.sum(
        returned.astype(jnp.float32).reshape(EXPERTS, shards, CAP, model_width), axis=1
    )
    summed = summed.reshape(EXPERTS * CAP, model_width)
    gathered = jnp.dot(placed, summed, precision=lax.Precision.HIGHEST)
    token_grad = jnp.sum(gathered.reshape(token_count, TOP, model_width), axis=1).astype(
        jnp.bfloat16
    )
    weight_grads = None
    for piece, (own_grads, their_grads) in enumerate(pairs):
        weight_grads = weight_pass(
            piece, pieces, weight_block, own_columns, their_columns, own_grads, their_grads,
            weight_grads,
        )
    gate_weight_grad, up_weight_grad = weight_grads
    return (token_grad, gate_weight_grad, up_weight_grad)


def solution(mesh):
    in_specs = (
        P(("dp", "expert"), None),
        P(("dp", "expert"), None),
        P(("dp", "expert"), None),
        P(None, "expert"),
        P(None, "expert"),
    )
    out_specs = (P(("dp", "expert"), None), P("dp", "expert"), P("dp", "expert"))
    return jax.shard_map(layer, mesh=mesh, in_specs=in_specs, out_specs=out_specs, check_vma=False)
```
